32 devices in a mesh: mem: 4 (over y, x), tile: 8 (over z, core).
Axes of the slice: x: 2, y: 2, z: 4, core: 2. Of those that a mesh axis runs over, the one named last changes fastest.
Arguments:
- perturbations: bfloat16 [3, 256, 128, 256], P(None, 'mem', 'tile'), may hold values from -0.375 to 0.375
- control: float32 [256, 128, 256], P('mem', 'tile'), may hold values from -15 to 15
- innovation: float32 [3, 128, 256], P(None, 'tile'), may hold values from -6 to 6
- obs_weight: float32 [3, 128, 256], P(None, 'tile'), may hold values from 2 to 32
- diffusion: float32 [128, 256], P('tile'), may hold values from 0.04 to 0.18
- advection: float32 [128, 256], P('tile'), may hold values from 0.08 to 0.3
- upwind: int32 [128, 256], P('tile'), may hold values from 0 to 1
Outputs:
- gradient: float32 [256, 128, 256], P('mem', 'tile')
- hessian_product: float32 [256, 128, 256], P('mem', 'tile')
- step_length: float32 [], replicated
The draws below stay inside these ranges and needn't reach their ends.
All inputs are finite; a program needn't handle non-finite values.
Results may differ from the reference program's by a relative error of at most 0.0003.
Values sent between devices are 32-bit elements; how exact they have to be, the bound alone decides.
No kernel may reach another device: no remote copies, remote signals or barrier semaphores. Data moves between devices by JAX's collectives and lax.ppermute only.
A program may use at most 64 MiB of HBM per device.

```python
import math
import jax
import jax.numpy as jnp
from jax import lax

M = 256
NT = 3
SWEEPS = 4
NY = 256
NX = 128


def draw_control(key, part):
    member_pos = jnp.arange(M, dtype=jnp.float32)[:, None, None] / M
    row_pos = jnp.arange(NX, dtype=jnp.float32)[None, :, None] / NX
    base = jax.random.truncated_normal(key, -5.0, 5.0, (M, NX, NY), jnp.float32)
    scale = jnp.sqrt((1.0 + 2.0 * member_pos) * (1.0 + 2.0 * row_pos))
    return (base * scale).astype(jnp.float32)


def plant(entries, stream_key, least, high):
    dims = entries.shape
    place = [jax.random.randint(jax.random.fold_in(stream_key, axis), (), 0, dims[axis]) for axis in range(len(dims))]
    entries = entries.at[tuple(place)].set(least)
    longest = dims.index(max(dims))
    place[longest] = (place[longest] + 1) % dims[longest]
    return entries.at[tuple(place)].set(high)


def block_levels(stream_key, extent, cuts, least, high):
    level = 1.0
    for axis_at, parts in cuts:
        heights = jax.random.uniform(jax.random.fold_in(jax.random.fold_in(stream_key, 6), axis_at), (parts,), jnp.float32, least / len(cuts), high / len(cuts))
        level = level * jnp.repeat(jnp.exp(heights), extent[axis_at] // parts).reshape((-1,) + (1,) * (len(extent) - 1 - axis_at))
    return level


def gaussian(stream_key, dims, width, most, split=(), kind=jnp.bfloat16):
    result = jax.random.normal(stream_key, dims, jnp.float32) * width
    if len(split) > 0:
        result = block_levels(stream_key, dims, split, -0.22, 0.18) * result
    return jnp.clip(result, min=-most, max=most).astype(kind)


def setup_inputs(seed: int = 0) -> dict:
    streams_of = jax.random.split(jax.random.key(seed), 8)
    return {
        "perturbations": gaussian(streams_of[0], (NT, M, NX, NY), M ** -0.5, 0.375, ((1, 4), (2, 8))),
        "control": draw_control(jax.random.fold_in(streams_of[7], 71), 0),
        "innovation": gaussian(streams_of[2], (NT, NX, NY), 1.0, 6.0, ((1, 8),), jnp.float32),
        "obs_weight": jnp.clip(jnp.exp(math.log(32.0) - 2.7725887 * jax.random.uniform(streams_of[3], (NT, NX, NY), jnp.float32) ** block_levels(streams_of[3], (NT, NX, NY), ((1, 8),), -0.2, 0.2)), 2.0, 32.0),
        "diffusion": jnp.clip(0.04 + 0.14000001 * jax.random.uniform(streams_of[4], (NX, NY), jnp.float32) ** block_levels(streams_of[4], (NX, NY), ((0, 8),), -0.2, 0.2), 0.04, 0.18),
        "advection": jnp.clip(0.08 + 0.22000001 * jax.random.uniform(streams_of[5], (NX, NY), jnp.float32) ** block_levels(streams_of[5], (NX, NY), ((0, 8),), -0.2, 0.2), 0.08, 0.3),
        "upwind": plant(jax.random.randint(streams_of[6], (NX, NY), 0, 2), jax.random.fold_in(streams_of[6], 1), 0, 1).astype(jnp.int32),
    }


member_block = 8


def pad_cells(values):
    widths = [(0, 0)] * (values.ndim - 2) + [(1, 1), (1, 1)]
    return jnp.pad(values, widths)


def forward_sweep(values, kappa_field, advect_field, upwind_field):
    padded = pad_cells(values)
    below = padded[..., 2:, 1:-1]
    above = padded[..., :-2, 1:-1]
    spread = below + above + padded[..., 1:-1, 2:] + padded[..., 1:-1, :-2] - 4.0 * values
    upwind_value = jnp.where(upwind_field == 1, below, above)
    return values + kappa_field * spread - advect_field * (values - upwind_value)


def adjoint_sweep(values, kappa_field, advect_field, upwind_field):
    weighted = kappa_field * values
    carried = advect_field * values
    to_lower = jnp.where(upwind_field == 0, carried, 0.0)
    to_upper = jnp.where(upwind_field == 1, carried, 0.0)
    padded = pad_cells(weighted)
    spread = padded[..., 2:, 1:-1] + padded[..., :-2, 1:-1] + padded[..., 1:-1, 2:] + padded[..., 1:-1, :-2] - 4.0 * weighted
    returned = pad_cells(to_lower)[..., 2:, 1:-1] + pad_cells(to_upper)[..., :-2, 1:-1]
    return values + spread - carried + returned


def reference(perturbations, control, innovation, obs_weight, diffusion, advection, upwind):
    groups = M // member_block
    pert_groups = jnp.moveaxis(perturbations.reshape(NT, groups, member_block, NX, NY), 1, 0)
    ctrl_groups = control.reshape(groups, member_block, NX, NY)

    def localise(values):
        for repeat in range(SWEEPS):
            values = forward_sweep(values, diffusion, advection, upwind)
        return values

    def localise_adjoint(values):
        for repeat in range(SWEEPS):
            values = adjoint_sweep(values, diffusion, advection, upwind)
        return values

    def project(field_groups):
        def one_group(inputs_pair):
            members, pert_block = inputs_pair
            spread_out = localise(members)
            return jnp.sum(pert_block.astype(jnp.float32) * spread_out[None], axis=1)
        return jnp.sum(lax.map(one_group, (field_groups, pert_groups)), axis=0)

    def adjoint(field_groups, weights_time):
        def one_group(inputs_pair):
            members, pert_block = inputs_pair
            pulled = jnp.sum(pert_block.astype(jnp.float32) * weights_time[:, None], axis=0)
            return members + localise_adjoint(pulled)
        return lax.map(one_group, (field_groups, pert_groups))

    increment = project(ctrl_groups)
    misfit = obs_weight * (increment - innovation)
    grad_groups = adjoint(ctrl_groups, misfit)
    image = project(grad_groups)
    weighted_image = obs_weight * image
    hess_groups = adjoint(grad_groups, weighted_image)
    gradient = grad_groups.reshape(M, NX, NY)
    hessian_product = hess_groups.reshape(M, NX, NY)
    squares = jnp.sum(gradient * gradient)
    curvature = squares + jnp.sum(image * weighted_image)
    return gradient, hessian_product, squares / curvature
```

```python
import jax
import jax.numpy as jnp
from jax import lax
from jax.sharding import PartitionSpec as P

SWEEPS = 4


def pairs_inner(count):
    return [(i, i ^ 1) for i in range(count) if (i ^ 1) < count]


def pairs_outer(count):
    partner = [(i, i + 1 if i % 2 else i - 1) for i in range(count)]
    return [(i, j) for i, j in partner if 0 <= j < count]


def halo(block, width, dim):
    count = lax.axis_size("tile")
    odd = lax.axis_index("tile") % 2 == 1
    top = lax.slice_in_dim(block, 0, width, axis=dim)
    bottom = lax.slice_in_dim(block, block.shape[dim] - width, None, axis=dim)
    outer = lax.ppermute(jnp.where(odd, bottom, top), "tile", pairs_outer(count))
    inner = lax.ppermute(jnp.where(odd, top, bottom), "tile", pairs_inner(count))
    return jnp.where(odd, inner, outer), jnp.where(odd, outer, inner)


def extended(block, width, dim):
    low, high = halo(block, width, dim)
    return jnp.concatenate([low, block, high], axis=dim)


def sum_over(value, axis):
    count = lax.axis_size(axis)
    power = count & (count - 1) == 0
    total = value
    for step in range(1, count):
        pairs = [(i, i ^ step if power else (i + step) % count) for i in range(count)]
        total = total + lax.ppermute(value, axis, pairs)
    return total


def sum_doubling(value, axis):
    count = lax.axis_size(axis)
    if count & (count - 1):
        return sum_over(value, axis)
    step = 1
    while step < count:
        value = value + lax.ppermute(value, axis, [(i, i ^ step) for i in range(count)])
        step *= 2
    return value


def column_pad(values):
    return jnp.pad(values, ((0, 0), (0, 0), (1, 1)))


def forward_core(extended, kappa_rows, advect_rows, upper_rows):
    center = extended[:, 1:-1]
    below = extended[:, 2:]
    above = extended[:, :-2]
    padded = column_pad(center)
    spread = below + above + padded[:, :, 2:] + padded[:, :, :-2] - 4.0 * center
    upwind_value = jnp.where(upper_rows, below, above)
    return center + kappa_rows * spread - advect_rows * (center - upwind_value)


def adjoint_core(center, carried, weighted_ext, lower_ext, upper_ext):
    weighted = weighted_ext[:, 1:-1]
    padded = column_pad(weighted)
    spread = (
        weighted_ext[:, 2:]
        + weighted_ext[:, :-2]
        + padded[:, :, 2:]
        + padded[:, :, :-2]
        - 4.0 * weighted
    )
    returned = lower_ext[:, 2:] + upper_ext[:, :-2]
    return center + spread - carried + returned


def shards(perturbations, control, innovation, obs_weight, diffusion, advection, upwind):
    row_count = control.shape[1]
    upper = upwind == 1
    stacked_coeff = jnp.stack([diffusion, advection, upper.astype(jnp.float32)])
    coefficients = extended(stacked_coeff, SWEEPS, 1)
    kappa_wide = coefficients[0]
    advect_wide = coefficients[1]
    upper_wide = coefficients[2] > 0.5
    global_rows = (
        lax.axis_index("tile") * row_count
        + jnp.arange(row_count + 2 * SWEEPS, dtype=jnp.int32)
        - SWEEPS
    )
    inside = ((global_rows >= 0) & (global_rows < row_count * lax.axis_size("tile"))).astype(
        jnp.float32
    )[:, None]

    def localise(values):
        wide = extended(values, SWEEPS, 1)
        for repeat in range(SWEEPS):
            first_row = repeat + 1
            last_row = row_count + 2 * SWEEPS - repeat - 1
            wide = (
                forward_core(
                    wide,
                    kappa_wide[first_row:last_row],
                    advect_wide[first_row:last_row],
                    upper_wide[first_row:last_row],
                )
                * inside[first_row:last_row]
            )
        return wide

    def localise_adjoint(values):
        wide = extended(values, SWEEPS, 1)
        for repeat in range(SWEEPS):
            last_row = row_count + 2 * SWEEPS - repeat
            upper_part = upper_wide[repeat:last_row]
            carried = advect_wide[repeat:last_row] * wide
            weighted = kappa_wide[repeat:last_row] * wide
            lower_ext = jnp.where(upper_part, 0.0, carried)
            upper_ext = jnp.where(upper_part, carried, 0.0)
            wide = (
                adjoint_core(wide[:, 1:-1], carried[:, 1:-1], weighted, lower_ext, upper_ext)
                * inside[repeat + 1 : last_row - 1]
            )
        return wide

    def project(values):
        return jnp.sum(perturbations.astype(jnp.float32) * values[None], axis=1)

    def pull_back(weights_time):
        return jnp.sum(perturbations.astype(jnp.float32) * weights_time[:, None], axis=0)

    increment = sum_over(project(localise(control)), "mem")
    misfit = obs_weight * (increment - innovation)
    gradient = control + localise_adjoint(pull_back(misfit))
    partial = project(localise(gradient))
    squares = jnp.sum(gradient * gradient, axis=(0, 1))
    times = partial.shape[0]
    flat = jnp.concatenate(
        [partial.reshape(times * row_count, -1), jnp.broadcast_to(squares / 8, (8,) + squares.shape)]
    )
    flat = sum_over(flat, "mem")
    image = flat[: times * row_count].reshape(partial.shape)
    weighted_image = obs_weight * image
    terms = image * weighted_image
    curve = terms.reshape(-1, 8, terms.shape[-1]).sum(0)
    both = sum_doubling(jnp.concatenate([flat[times * row_count :], curve]), "tile")
    square_sum = jnp.sum(both[:8])
    hessian_product = gradient + localise_adjoint(pull_back(weighted_image))
    return (gradient, hessian_product, square_sum / (square_sum + jnp.sum(both[8:])))


def solution(mesh):
    return jax.shard_map(
        shards,
        mesh=mesh,
        in_specs=(
            P(None, "mem", "tile", None),
            P("mem", "tile", None),
            P(None, "tile", None),
            P(None, "tile", None),
            P("tile", None),
            P("tile", None),
            P("tile", None),
        ),
        out_specs=(P("mem", "tile", None), P("mem", "tile", None), P()),
        check_vma=False,
    )
```

```python
import jax
import jax.numpy as jnp
from jax import lax
from jax.experimental import pallas as pl
from jax.experimental.pallas import tpu as pltpu
from jax.sharding import PartitionSpec as P

SWEEPS = 4
SUB = 8
CHUNKS = 4
VMEM_BYTES = 67043328
SPARE = 3072
LANES = 128
PACK = 1
GROUP = 8


def pairs_inner(count):
    return [(i, i ^ 1) for i in range(count) if (i ^ 1) < count]


def pairs_outer(count):
    partner = [(i, i + 1 if i % 2 else i - 1) for i in range(count)]
    return [(i, j) for i, j in partner if 0 <= j < count]


def swap(inner, outer):
    count = lax.axis_size("tile")
    far = lax.ppermute(outer, "tile", pairs_outer(count))
    near = lax.ppermute(inner, "tile", pairs_inner(count))
    return near, far


def others(value, axis, stride=1):
    count = lax.axis_size(axis)
    power = count & (count - 1) == 0
    return [
        lax.ppermute(
            value, axis, [(i, i ^ step if power else (i + step) % count) for i in range(count)]
        )
        for step in range(stride, count, stride)
    ]


def order(width, back):
    wide = PACK * width
    cols, each = wide // LANES, LANES // PACK
    a = jnp.arange(wide, dtype=jnp.int32)
    lane, vector = a % LANES, a // LANES
    source = (lane // each) * width + cols * (lane % each) + vector
    if back:
        return (source[:, None] == a[None, :]).astype(jnp.bfloat16)
    return (a[:, None] == source[None, :]).astype(jnp.bfloat16)


def order_matrix(width):
    wide = PACK * width
    cols, each = wide // LANES, LANES // PACK
    a = lax.broadcasted_iota(jnp.int32, (wide, wide), 1)
    lane, vector = a % LANES, a // LANES
    source = (lane // each) * width + cols * (lane % each) + vector
    return jnp.where(lax.broadcasted_iota(jnp.int32, (wide, wide), 0) == source, 1.0, 0.0).astype(
        jnp.bfloat16
    )


def reordered(x, matrix):
    out = None
    for part in range(3):
        piece = x.astype(jnp.bfloat16)
        term = jnp.dot(piece, matrix, preferred_element_type=jnp.float32)
        out = term if out is None else out + term
        x = x - piece.astype(jnp.float32)
    return out


def columns(c):
    return pl.ds(c * LANES, LANES)


def sides(values, lane):
    last, each = len(values) - 1, LANES // PACK
    right = jnp.where(lane % each == each - 1, 0.0, pltpu.roll(values[0], LANES - 1, 1))
    left = jnp.where(lane % each == 0, 0.0, pltpu.roll(values[last], 1, 1))
    around = [left] + list(values) + [right]
    return [around[c] + around[c + 2] for c in range(last + 1)]


def below_of(x):
    return x[1:] + [pltpu.roll(x[0], SUB - 1, 0)]


def above_of(x):
    return [pltpu.roll(x[-1], 1, 0)] + x[:-1]


def forward(x, coef, lane):
    cols, tiles = len(x), len(x[0])
    lateral = [sides([x[c][t] for c in range(cols)], lane) for t in range(tiles)]
    out = []
    for c in range(cols):
        below, above = below_of(x[c]), above_of(x[c])
        out.append(
            [
                coef[0, c, t] * x[c][t]
                + coef[1, c, t] * below[t]
                + coef[2, c, t] * above[t]
                + coef[3, c, t] * lateral[t][c]
                for t in range(tiles)
            ]
        )
    return out


def adjoint(x, coef, lane):
    cols, tiles = len(x), len(x[0])
    lateral = [
        sides([coef[3, c, t] * x[c][t] for c in range(cols)], lane) for t in range(tiles)
    ]
    out = []
    for c in range(cols):
        below = below_of([coef[2, c, t] * x[c][t] for t in range(tiles)])
        above = above_of([coef[1, c, t] * x[c][t] for t in range(tiles)])
        out.append(
            [
                coef[0, c, t] * x[c][t] + below[t] + above[t] + lateral[t][c]
                for t in range(tiles)
            ]
        )
    return out


def sweeps(step, rows_ref, g, coef, lane, cols, tiles):
    x = [
        [rows_ref[g, c, pl.ds(t, SUB, stride=tiles), :] for t in range(tiles)]
        for c in range(cols)
    ]
    for _ in range(SWEEPS):
        x = step(x, coef, lane)
    for c in range(cols):
        for t in range(tiles):
            rows_ref[g, c, pl.ds(t, SUB, stride=tiles), :] = x[c][t]


def lane_of():
    return lax.broadcasted_iota(jnp.int32, (SUB, LANES), 1)


def sub_of():
    return lax.broadcasted_iota(jnp.int32, (SUB, LANES), 0)


def is_odd():
    return lax.axis_index("tile") % 2 == 1


def call(kernel, outs, scratch, operands, near=None, flops=1, limit=24 * 2**20):
    near = len(operands) if near is None else len(operands) + near
    nbytes = sum(x.size * x.dtype.itemsize for x in operands)
    return pl.pallas_call(
        kernel,
        out_shape=outs,
        in_specs=[
            pl.BlockSpec(memory_space=pltpu.VMEM if k < near else pl.ANY)
            for k in range(len(operands))
        ],
        out_specs=[pl.BlockSpec(memory_space=pltpu.VMEM)] * len(outs),
        scratch_shapes=scratch,
        compiler_params=pltpu.CompilerParams(vmem_limit_bytes=limit),
        cost_estimate=pl.CostEstimate(flops=flops, bytes_accessed=nbytes, transcendentals=0),
    )(*operands)


def f32(*shape):
    return jax.ShapeDtypeStruct(shape, jnp.float32)


def edge_kernel(members, control, diffusion, advection, upwind, near, far, fields, buf, number,
                stage, sems):
    _, rows, width = control.shape
    chunk = members // CHUNKS
    copies = [
        pltpu.make_async_copy(
            control.at[pl.ds(i * chunk, chunk)], buf.at[pl.ds(i * chunk, chunk)], sems.at[i]
        )
        for i in range(CHUNKS)
    ] + [
        pltpu.make_async_copy(diffusion, fields.at[0], sems.at[CHUNKS]),
        pltpu.make_async_copy(advection, fields.at[1], sems.at[CHUNKS + 1]),
        pltpu.make_async_copy(upwind, number, sems.at[CHUNKS + 2]),
    ]
    for copy in copies[CHUNKS:] + copies[:CHUNKS]:
        copy.start()
    odd, turn = is_odd(), order_matrix(width)
    sub = lax.broadcasted_iota(jnp.int32, (SUB, width), 0)
    last = pl.ds(rows - SUB, SUB)
    for copy in copies[CHUNKS:]:
        copy.wait()
    fields[2] = number[...].astype(jnp.float32)
    for q in range(3):
        top, end = fields[q, pl.ds(0, SUB), :], fields[q, last, :]
        at = pl.ds(members // PACK * SWEEPS + q * SUB, SUB)
        for b in range(PACK):
            cs = pl.ds(b * width, width)
            stage[0, at, cs] = jnp.where(odd, top, end)
            stage[1, at, cs] = jnp.where(odd, end, top)
    pairs = chunk // (2 * PACK)
    for k in range(members // (2 * PACK)):
        if k % pairs == 0:
            copies[k // pairs].wait()
        at = pl.ds(k * SUB, SUB)
        for b in range(PACK):
            first, second = 2 * PACK * k + b, 2 * PACK * k + PACK + b
            cs = pl.ds(b * width, width)
            x, y = buf[first, pl.ds(0, SUB), :], buf[second, pl.ds(0, SUB), :]
            top = jnp.where(sub < SWEEPS, x, pltpu.roll(y, SWEEPS, 0))
            x, y = buf[first, last, :], buf[second, last, :]
            end = jnp.where(sub < SWEEPS, pltpu.roll(x, SWEEPS, 0), y)
            stage[0, at, cs] = jnp.where(odd, top, end)
            stage[1, at, cs] = jnp.where(odd, end, top)
    near[...] = reordered(stage[0], turn)
    far[...] = reordered(stage[1], turn)


def side_by_side(parts):
    return jnp.concatenate(
        [jnp.concatenate(parts[i : i + PACK], 1) for i in range(0, len(parts), PACK)], 0
    )


def order_kernel(times, members, control, fields, pert, matrix, control_out, fields_out, pert_out):
    _, rows, width = control.shape
    turn = matrix[...]
    chunk = 2 * GROUP * PACK

    def group(step, carry):
        out = pl.ds(step * 2 * GROUP, 2 * GROUP)
        block = side_by_side([control[step * chunk + k] for k in range(chunk)])
        control_out[out] = reordered(block, turn).reshape((2 * GROUP,) + control_out.shape[1:])
        block = side_by_side(
            [pert[t, step * chunk + k] for t in range(times) for k in range(chunk)]
        )
        turned = jnp.dot(block, turn, preferred_element_type=jnp.float32).astype(jnp.bfloat16)
        turned = turned.reshape((times, 2 * GROUP) + pert_out.shape[2:])
        for t in range(times):
            pert_out[t, out] = turned[t]
        return carry

    lax.fori_loop(0, members // chunk, group, 0)
    plane_kernel(fields, matrix, fields_out)


def plane_kernel(*refs):
    count = len(refs) // 2
    turn = refs[count][...]
    for ref, out in zip(refs[:count], refs[count + 1 :]):
        block = ref[...].reshape(ref.shape[0] * ref.shape[1], ref.shape[2])
        out[...] = reordered(jnp.concatenate([block] * PACK, 1), turn).reshape(out.shape)


def restore_packs(first, count, field, turn, out):
    rows, width = out.shape[1:]
    block = field[pl.ds(first, count)].reshape(count * rows, PACK * width)
    block = reordered(block, turn)
    for k in range(count):
        for b in range(PACK):
            out[(first + k) * PACK + b] = block[
                k * rows : (k + 1) * rows, b * width : (b + 1) * width
            ]


def restore_kernel(packs, field, matrix, out, token):
    turn = matrix[...]
    token[...] = jnp.zeros_like(token)

    def group(step, carry):
        restore_packs(step * 4 * GROUP, 4 * GROUP, field, turn, out)
        return carry

    lax.fori_loop(0, packs // (4 * GROUP), group, 0)


def coefficients_into(fields, halo_low, halo_high, base, out3, out4, ring, dims):
    cols, own = dims
    sub = sub_of()
    fields3, fields4 = [], []
    for q in range(3):
        for c in range(cols):
            for i in range(own):
                ring[0, c, pl.ds(i * SUB, SUB), :] = fields[q, pl.ds(i * SUB, SUB), columns(c)]
            high = halo_high(base + q * SUB, c)
            low = halo_low(base + q * SUB, c)
            ring[0, c, pl.ds(own * SUB, SUB), :] = high
            ring[0, c, pl.ds((own + 1) * SUB, SUB), :] = low
            n = own + 2
            fields4.append([ring[0, c, pl.ds(t, SUB, stride=n), :] for t in range(n)])
            ring[0, c, pl.ds(own * SUB, SUB), :] = jnp.where(sub < SWEEPS, high, low)
            n = own + 1
            fields3.append([ring[0, c, pl.ds(t, SUB, stride=n), :] for t in range(n)])
    for fields, out in ((fields3, out3), (fields4, out4)):
        for c in range(cols):
            for t in range(len(fields[0])):
                kappa, advect, upper = (fields[q * cols + c][t] for q in range(3))
                toward = advect * upper
                out[0, c, t] = 1.0 - 4.0 * kappa - advect
                out[1, c, t] = kappa + toward
                out[2, c, t] = kappa + (advect - toward)
                out[3, c, t] = kappa


def project_member(pert, m, rows_ref, g, total, dims):
    cols, own = dims
    out = [[list(col) for col in per_time] for per_time in total]
    for c in range(cols):
        field = [rows_ref[g, c, pl.ds(i * SUB, SUB), :] for i in range(own)]
        for t in range(len(total)):
            weight = pert[t, m, :, columns(c)].astype(jnp.float32)
            for i in range(own):
                out[t][c][i] = total[t][c][i] + weight[i * SUB : (i + 1) * SUB] * field[i]
    return out


def zeros(times, dims):
    cols, own = dims
    zero = jnp.zeros((SUB, LANES), jnp.float32)
    return [[[zero] * own for _ in range(cols)] for _ in range(times)]


def write_sums(ref, total, dims, lane):
    cols, own = dims
    half = LANES // PACK
    for t, per_time in enumerate(total):
        for c in range(0, cols, PACK):
            for i in range(own):
                if PACK == 1:
                    ref[pl.ds((t * own + i) * SUB, SUB), columns(c)] = per_time[c][i]
                    continue
                x, y = (per_time[c + b][i] for b in range(PACK))
                x, y = x + pltpu.roll(x, half, 1), y + pltpu.roll(y, half, 1)
                ref[pl.ds((t * own + i) * SUB, SUB), columns(c // PACK)] = jnp.where(
                    lane < half, x, y
                )


def first_kernel(dims, times, members, control, near, far, fields, pert, sums, out3,
                 out4, halo, ring):
    cols, own = dims
    lane, sub, odd = lane_of(), sub_of(), is_odd()

    def high_of(start, c):
        rows = pl.ds(start, SUB)
        return jnp.where(odd, far[rows, columns(c)], near[rows, columns(c)])

    def low_of(start, c):
        rows = pl.ds(start, SUB)
        return jnp.where(odd, near[rows, columns(c)], far[rows, columns(c)])

    coefficients_into(
        fields, low_of, high_of, members * SWEEPS, out3, out4, ring, dims
    )

    def group(step, total):
        for pair in range(GROUP // 2):
            first = step * GROUP + 2 * pair
            start = pl.multiple_of(first * SWEEPS, SUB)
            for c in range(cols):
                high, low = high_of(start, c), low_of(start, c)
                edges = (
                    jnp.where(sub < SWEEPS, high, pltpu.roll(low, SWEEPS, 0)),
                    jnp.where(sub < SWEEPS, pltpu.roll(high, SWEEPS, 0), low),
                )
                for k in range(2):
                    g = 2 * pair + k
                    for i in range(own):
                        rows = pl.ds(i * SUB, SUB)
                        ring[g, c, rows, :] = control[first + k, rows, columns(c)]
                    ring[g, c, pl.ds(own * SUB, SUB), :] = edges[k]
                    halo[first + k, :, columns(c)] = edges[k]
        for g in range(GROUP):
            sweeps(forward, ring, g, out3, lane, cols, own + 1)
            total = project_member(pert, step * GROUP + g, ring, g, total, dims)
        return total

    total = lax.fori_loop(0, members // GROUP, group, zeros(times, dims))
    write_sums(sums, total, dims, lane)


def pull_member(pert, m, weights, c, own):
    out = None
    for t in range(len(weights)):
        value = pert[t, m, :, columns(c)].astype(jnp.float32)
        terms = [value[i * SUB : (i + 1) * SUB] * weights[t][c][i] for i in range(own)]
        out = terms if out is None else [a + b for a, b in zip(out, terms)]
    return out


def gathered(parts, rows, c):
    out = parts[0][rows, columns(c)]
    for part in parts[1:]:
        out = out + part[rows, columns(c)]
    return out


def totals_of(parts, t, i, dims, lane):
    cols, own = dims
    half = LANES // PACK
    out = []
    for c in range(cols // PACK):
        x = gathered(parts, pl.ds((t * own + i) * SUB, SUB), c)
        if PACK == 1:
            out.append(x)
            continue
        y = pltpu.roll(x, half, 1)
        out += [jnp.where(lane < half, x, y), jnp.where(lane < half, y, x)]
    return out


def second_kernel(dims, times, members, count, *refs):
    cols, own = dims
    parts, (innovation, weight, pert, near, far, rest) = refs[:count], refs[count:]
    odd, lane = is_odd(), lane_of()
    weights = []
    for t in range(times):
        weights.append([[None] * own for _ in range(cols)])
        for i in range(own):
            rows = pl.ds(i * SUB, SUB)
            total = totals_of(parts, t, i, dims, lane)
            for c in range(cols):
                weights[t][c][i] = weight[t, rows, columns(c)] * (
                    total[c] - innovation[t, rows, columns(c)]
                )

    def group(step, carry):
        for g in range(GROUP):
            m = step * GROUP + g
            for c in range(cols):
                tiles = pull_member(pert, m, weights, c, own)
                near[m, :, columns(c)] = jnp.where(odd, tiles[0], tiles[-1])
                far[m, :, columns(c)] = jnp.where(odd, tiles[-1], tiles[0])
                for i in range(1, own - 1):
                    rest[m, pl.ds((i - 1) * SUB, SUB), columns(c)] = tiles[i]
        return carry

    lax.fori_loop(0, members // GROUP, group, 0)


def third_kernel(dims, times, members, control, halo, near, far, rest, from_near, from_far,
                 coef3, coef4, pert, gradient, sums, ring, ring3):
    cols, own = dims
    lane, sub, odd = lane_of(), sub_of(), is_odd()
    index = lax.axis_index("tile")
    inside = jnp.where(
        sub < SWEEPS,
        jnp.where(index < lax.axis_size("tile") - 1, 1.0, 0.0),
        jnp.where(index > 0, 1.0, 0.0),
    )

    def group(step, carry):
        total, square = carry
        for g in range(GROUP):
            m = step * GROUP + g
            for c in range(cols):
                cs = columns(c)
                a, b = near[m, :, cs], far[m, :, cs]
                ring[g, c, pl.ds(0, SUB), :] = jnp.where(odd, a, b)
                ring[g, c, pl.ds((own - 1) * SUB, SUB), :] = jnp.where(odd, b, a)
                for i in range(1, own - 1):
                    ring[g, c, pl.ds(i * SUB, SUB), :] = rest[m, pl.ds((i - 1) * SUB, SUB), cs]
                a, b = from_near[m, :, cs], from_far[m, :, cs]
                ring[g, c, pl.ds(own * SUB, SUB), :] = jnp.where(odd, b, a)
                ring[g, c, pl.ds((own + 1) * SUB, SUB), :] = jnp.where(odd, a, b)
        for g in range(GROUP):
            m = step * GROUP + g
            sweeps(adjoint, ring, g, coef4, lane, cols, own + 2)
            for c in range(cols):
                cs = columns(c)
                for i in range(own):
                    rows = pl.ds(i * SUB, SUB)
                    value = control[m, rows, cs] + ring[g, c, rows, :]
                    gradient[m, rows, cs] = value
                    ring3[g, c, rows, :] = value
                    square = square + value * value
                edge = jnp.where(
                    sub < SWEEPS,
                    ring[g, c, pl.ds(own * SUB, SUB), :],
                    ring[g, c, pl.ds((own + 1) * SUB, SUB), :],
                )
                ring3[g, c, pl.ds(own * SUB, SUB), :] = inside * (halo[m, :, cs] + edge)
            sweeps(forward, ring3, g, coef3, lane, cols, own + 1)
            total = project_member(pert, m, ring3, g, total, dims)
        return total, square

    total, square = lax.fori_loop(
        0,
        members // GROUP,
        group,
        (zeros(times, dims), jnp.zeros((SUB, LANES), jnp.float32)),
    )
    write_sums(sums, total, dims, lane)
    sums[pl.ds(times * own * SUB, SUB), :] = jnp.zeros((SUB, sums.shape[1]), jnp.float32)
    sums[pl.ds(times * own * SUB, SUB), columns(0)] = square


def fourth_kernel(dims, times, members, count, *refs):
    cols, own = dims
    parts, (weight, pert, _, field, near, far) = refs[:count], refs[count:]
    odd, sub, lane = is_odd(), sub_of(), lane_of()
    weights = []
    curve = jnp.zeros((SUB, LANES), jnp.float32)
    for t in range(times):
        weights.append([[None] * own for _ in range(cols)])
        for i in range(own):
            total = totals_of(parts, t, i, dims, lane)
            for c in range(cols):
                weights[t][c][i] = weight[t, pl.ds(i * SUB, SUB), columns(c)] * total[c]
                curve = curve + total[c] * weights[t][c][i]
    square = gathered(parts, pl.ds(times * own * SUB, SUB), 0)
    base = members * SWEEPS
    near[pl.ds(base, 2 * SUB), :] = jnp.zeros((2 * SUB, near.shape[1]), jnp.float32)
    near[pl.ds(base, SUB), columns(0)] = square
    near[pl.ds(base + SUB, SUB), columns(0)] = curve * (1.0 / PACK)

    def group(step, carry):
        for pair in range(GROUP // 2):
            first = step * GROUP + 2 * pair
            start = pl.multiple_of(first * SWEEPS, SUB)
            for c in range(cols):
                cs = columns(c)
                both = []
                for k in range(2):
                    tiles = pull_member(pert, first + k, weights, c, own)
                    for i in range(own):
                        field[first + k, pl.ds(i * SUB, SUB), cs] = tiles[i]
                    both.append(tiles)
                top = jnp.where(sub < SWEEPS, both[0][0], pltpu.roll(both[1][0], SWEEPS, 0))
                end = jnp.where(sub < SWEEPS, pltpu.roll(both[0][-1], SWEEPS, 0), both[1][-1])
                near[pl.ds(start, SUB), cs] = jnp.where(odd, top, end)
                far[pl.ds(start, SUB), cs] = jnp.where(odd, end, top)
        return carry

    lax.fori_loop(0, members // GROUP, group, 0)


def fifth_kernel(dims, members, field, near, far, coef3, gradient, matrix, *refs):
    scalars, (product, length, ring, turned) = refs[:-4], refs[-4:]
    cols, own = dims
    lane, sub, odd = lane_of(), sub_of(), is_odd()
    turn = matrix[...]

    def group(step):
        for pair in range(GROUP // 2):
            first = step * GROUP + 2 * pair
            start = first * SWEEPS
            rows8 = pl.ds(start if isinstance(step, int) else pl.multiple_of(start, SUB), SUB)
            for c in range(cols):
                cs = columns(c)
                a, b = near[rows8, cs], far[rows8, cs]
                high, low = jnp.where(odd, b, a), jnp.where(odd, a, b)
                edges = (
                    jnp.where(sub < SWEEPS, high, pltpu.roll(low, SWEEPS, 0)),
                    jnp.where(sub < SWEEPS, pltpu.roll(high, SWEEPS, 0), low),
                )
                for k in range(2):
                    g = 2 * pair + k
                    for i in range(own):
                        rows = pl.ds(i * SUB, SUB)
                        ring[g, c, rows, :] = field[first + k, rows, cs]
                    ring[g, c, pl.ds(own * SUB, SUB), :] = edges[k]
        for g in range(GROUP):
            m = step * GROUP + g
            sweeps(adjoint, ring, g, coef3, lane, cols, own + 1)
            for c in range(cols):
                for i in range(own):
                    rows = pl.ds(i * SUB, SUB)
                    turned[m, rows, columns(c)] = (
                        gradient[m, rows, columns(c)] + ring[g, c, rows, :]
                    )

    def both(step, carry):
        restore_packs((step - 1) * GROUP, GROUP, turned, turn, product)
        group(step)
        return carry

    total = sum((ref[...] for ref in scalars[1:]), scalars[0][...])
    square = jnp.sum(total[:SUB], keepdims=True)
    length[...] = square / (square + jnp.sum(total[SUB:], keepdims=True))
    group(0)
    lax.fori_loop(1, members // GROUP, both, 0)
    restore_packs(members - GROUP, GROUP, turned, turn, product)


def bind(kernel, *static):
    def bound(*refs):
        kernel(*static, *refs)

    return bound


def shards(perturbations, control, innovation, obs_weight, diffusion, advection, upwind):
    times, members, rows, width = perturbations.shape
    packs, wide = members // PACK, PACK * width
    cols, own = wide // LANES, rows // SUB
    dims = (cols, own)

    turn, back = order(width, False), order(width, True)
    edge = f32(packs * SWEEPS + 3 * SUB, wide)
    planes = f32(3, rows, width)
    near, far, fields = call(
        bind(edge_kernel, members),
        [edge, edge, planes],
        [
            pltpu.VMEM(control.shape, jnp.float32),
            pltpu.VMEM((rows, width), jnp.int32),
            pltpu.VMEM((2,) + edge.shape, jnp.float32),
            pltpu.SemaphoreType.DMA((CHUNKS + 3,)),
        ],
        [control, diffusion, advection, upwind],
        near=-4,
        limit=VMEM_BYTES - 4 * (2 * edge.size + planes.size + SPARE),
    )
    near, far = swap(near, far)
    packed = f32(packs, rows, wide)
    per_time = f32(times, rows, wide)
    gradient_shape = f32(*control.shape)
    control, fields, perturbations = call(
        bind(order_kernel, times, members),
        [packed, f32(3, rows, wide), jax.ShapeDtypeStruct((times,) + packed.shape, jnp.bfloat16)],
        [],
        [control, fields, perturbations, turn],
        flops=2_000_000_000,
    )
    innovation, obs_weight = call(
        plane_kernel, [per_time, per_time], [], [innovation, obs_weight, turn], flops=200_000_000
    )

    def ring_of(n):
        return pltpu.VMEM((GROUP, cols, n * SUB, LANES), jnp.float32)

    sums, coef3, coef4, halo = call(
        bind(first_kernel, dims, times, packs),
        [
            f32(times * rows, width),
            f32(4, cols, own + 1, SUB, LANES),
            f32(4, cols, own + 2, SUB, LANES),
            f32(packs, SUB, wide),
        ],
        [ring_of(own + 2)],
        [control, near, far, fields, perturbations],
        flops=4_000_000_000,
    )
    parts = [sums] + others(sums, "mem")
    edges = f32(packs, SUB, wide)
    near, far, rest = call(
        bind(second_kernel, dims, times, packs, len(parts)),
        [edges, edges, f32(packs, max(own - 2, 1) * SUB, wide)],
        [],
        parts + [innovation, obs_weight, perturbations],
    )
    from_near, from_far = swap(near, far)
    gradient, sums = call(
        bind(third_kernel, dims, times, packs),
        [packed, f32(times * rows + SUB, width)],
        [ring_of(own + 2), ring_of(own + 1)],
        [control, halo, near, far, rest, from_near, from_far, coef3, coef4, perturbations],
        flops=8_000_000_000,
    )
    parts = [sums] + others(sums, "mem")
    restored, token = call(
        bind(restore_kernel, packs),
        [gradient_shape, f32(SUB, LANES)],
        [],
        [gradient, back],
        flops=1_000_000_000,
    )
    field, near, far = call(
        bind(fourth_kernel, dims, times, packs, len(parts)),
        [packed, f32(packs * SWEEPS + 2 * SUB, wide), f32(packs * SWEEPS, wide)],
        [],
        parts + [obs_weight, perturbations, token],
    )
    from_near, from_far = swap(near, far)
    one = near[packs * SWEEPS :, :LANES] + from_near[packs * SWEEPS :, :LANES]
    scalars = [one] + others(one, "tile", 2)
    product, length = call(
        bind(fifth_kernel, dims, packs),
        [gradient_shape, f32(1, 1)],
        [ring_of(own + 1), pltpu.VMEM(gradient.shape, jnp.float32)],
        [field, from_near, from_far, coef3, gradient, back] + scalars,
        flops=4_000_000_000,
    )
    return restored, product, length[0, 0]


def solution(mesh):
    return jax.shard_map(
        shards,
        mesh=mesh,
        in_specs=(
            P(None, "mem", "tile", None),
            P("mem", "tile", None),
            P(None, "tile", None),
            P(None, "tile", None),
            P("tile", None),
            P("tile", None),
            P("tile", None),
        ),
        out_specs=(P("mem", "tile", None), P("mem", "tile", None), P()),
        check_vma=False,
    )
```

```python
import jax
import jax.numpy as jnp
from jax import lax
from jax.experimental import pallas as pl
from jax.experimental.pallas import tpu as pltpu
from jax.sharding import PartitionSpec as P

SWEEPS = 4
SUB = 8
CHUNKS = 4
UNROLL = 7
VMEM_BYTES = 67043328
SPARE = 3072
LANES = 128
PACK = 1
GROUP = 8


def pairs_inner(count):
    return [(i, i ^ 1) for i in range(count) if (i ^ 1) < count]


def pairs_outer(count):
    partner = [(i, i + 1 if i % 2 else i - 1) for i in range(count)]
    return [(i, j) for i, j in partner if 0 <= j < count]


def swap(inner, outer):
    count = lax.axis_size("tile")
    far = lax.ppermute(outer, "tile", pairs_outer(count))
    near = lax.ppermute(inner, "tile", pairs_inner(count))
    return near, far


def others(value, axis, stride=1):
    count = lax.axis_size(axis)
    power = count & (count - 1) == 0
    return [
        lax.ppermute(
            value, axis, [(i, i ^ step if power else (i + step) % count) for i in range(count)]
        )
        for step in range(stride, count, stride)
    ]


def order(width, back):
    wide = PACK * width
    cols, each = wide // LANES, LANES // PACK
    a = jnp.arange(wide, dtype=jnp.int32)
    lane, vector = a % LANES, a // LANES
    source = (lane // each) * width + cols * (lane % each) + vector
    if back:
        return (source[:, None] == a[None, :]).astype(jnp.bfloat16)
    return (a[:, None] == source[None, :]).astype(jnp.bfloat16)


def order_matrix(width):
    wide = PACK * width
    cols, each = wide // LANES, LANES // PACK
    a = lax.broadcasted_iota(jnp.int32, (wide, wide), 1)
    lane, vector = a % LANES, a // LANES
    source = (lane // each) * width + cols * (lane % each) + vector
    return jnp.where(lax.broadcasted_iota(jnp.int32, (wide, wide), 0) == source, 1.0, 0.0).astype(
        jnp.bfloat16
    )


def reordered(x, matrix):
    high = x.astype(jnp.bfloat16)
    low = (x - high.astype(jnp.float32)).astype(jnp.bfloat16)
    return jnp.dot(high, matrix, preferred_element_type=jnp.float32) + jnp.dot(
        low, matrix, preferred_element_type=jnp.float32
    )


def columns(c):
    return pl.ds(c * LANES, LANES)


def sides(values, lane):
    last, each = len(values) - 1, LANES // PACK
    right = jnp.where(lane % each == each - 1, 0.0, pltpu.roll(values[0], LANES - 1, 1))
    left = jnp.where(lane % each == 0, 0.0, pltpu.roll(values[last], 1, 1))
    around = [left] + list(values) + [right]
    return [around[c] + around[c + 2] for c in range(last + 1)]


def below_of(x):
    return x[1:] + [pltpu.roll(x[0], SUB - 1, 0)]


def above_of(x):
    return [pltpu.roll(x[-1], 1, 0)] + x[:-1]


def forward(x, coef, lane):
    cols, tiles = len(x), len(x[0])
    lateral = [sides([x[c][t] for c in range(cols)], lane) for t in range(tiles)]
    out = []
    for c in range(cols):
        below, above = below_of(x[c]), above_of(x[c])
        out.append(
            [
                coef[0, c, t] * x[c][t]
                + coef[1, c, t] * below[t]
                + coef[2, c, t] * above[t]
                + coef[3, c, t] * lateral[t][c]
                for t in range(tiles)
            ]
        )
    return out


def adjoint(x, coef, lane):
    cols, tiles = len(x), len(x[0])
    lateral = [
        sides([coef[3, c, t] * x[c][t] for c in range(cols)], lane) for t in range(tiles)
    ]
    out = []
    for c in range(cols):
        below = below_of([coef[2, c, t] * x[c][t] for t in range(tiles)])
        above = above_of([coef[1, c, t] * x[c][t] for t in range(tiles)])
        out.append(
            [
                coef[0, c, t] * x[c][t] + below[t] + above[t] + lateral[t][c]
                for t in range(tiles)
            ]
        )
    return out


def sweeps(step, rows_ref, g, coef, lane, cols, tiles):
    x = [
        [rows_ref[g, c, pl.ds(t, SUB, stride=tiles), :] for t in range(tiles)]
        for c in range(cols)
    ]
    for _ in range(SWEEPS):
        x = step(x, coef, lane)
    for c in range(cols):
        for t in range(tiles):
            rows_ref[g, c, pl.ds(t, SUB, stride=tiles), :] = x[c][t]


def lane_of():
    return lax.broadcasted_iota(jnp.int32, (SUB, LANES), 1)


def sub_of():
    return lax.broadcasted_iota(jnp.int32, (SUB, LANES), 0)


def is_odd():
    return lax.axis_index("tile") % 2 == 1


def call(kernel, outs, scratch, operands, near=None, flops=1, limit=24 * 2**20):
    near = len(operands) if near is None else len(operands) + near
    nbytes = sum(x.size * x.dtype.itemsize for x in operands)
    return pl.pallas_call(
        kernel,
        out_shape=outs,
        in_specs=[
            pl.BlockSpec(memory_space=pltpu.VMEM if k < near else pl.ANY)
            for k in range(len(operands))
        ],
        out_specs=[pl.BlockSpec(memory_space=pltpu.VMEM)] * len(outs),
        scratch_shapes=scratch,
        compiler_params=pltpu.CompilerParams(vmem_limit_bytes=limit),
        cost_estimate=pl.CostEstimate(flops=flops, bytes_accessed=nbytes, transcendentals=0),
    )(*operands)


def f32(*shape):
    return jax.ShapeDtypeStruct(shape, jnp.float32)


def edge_kernel(members, control, diffusion, advection, upwind, near, far, fields, buf, number,
                stage, sems):
    _, rows, width = control.shape
    chunk = members // CHUNKS
    copies = [
        pltpu.make_async_copy(
            control.at[pl.ds(i * chunk, chunk)], buf.at[pl.ds(i * chunk, chunk)], sems.at[i]
        )
        for i in range(CHUNKS)
    ] + [
        pltpu.make_async_copy(diffusion, fields.at[0], sems.at[CHUNKS]),
        pltpu.make_async_copy(advection, fields.at[1], sems.at[CHUNKS + 1]),
        pltpu.make_async_copy(upwind, number, sems.at[CHUNKS + 2]),
    ]
    for copy in copies[CHUNKS:] + copies[:CHUNKS]:
        copy.start()
    odd, turn = is_odd(), order_matrix(width)
    sub = lax.broadcasted_iota(jnp.int32, (SUB, width), 0)
    last = pl.ds(rows - SUB, SUB)
    for copy in copies[CHUNKS:]:
        copy.wait()
    fields[2] = number[...].astype(jnp.float32)
    for q in range(3):
        top, end = fields[q, pl.ds(0, SUB), :], fields[q, last, :]
        at = pl.ds(members // PACK * SWEEPS + q * SUB, SUB)
        for b in range(PACK):
            cs = pl.ds(b * width, width)
            stage[0, at, cs] = jnp.where(odd, top, end)
            stage[1, at, cs] = jnp.where(odd, end, top)
    pairs = chunk // (2 * PACK)
    for k in range(members // (2 * PACK)):
        if k % pairs == 0:
            copies[k // pairs].wait()
        at = pl.ds(k * SUB, SUB)
        for b in range(PACK):
            first, second = 2 * PACK * k + b, 2 * PACK * k + PACK + b
            cs = pl.ds(b * width, width)
            x, y = buf[first, pl.ds(0, SUB), :], buf[second, pl.ds(0, SUB), :]
            top = jnp.where(sub < SWEEPS, x, pltpu.roll(y, SWEEPS, 0))
            x, y = buf[first, last, :], buf[second, last, :]
            end = jnp.where(sub < SWEEPS, pltpu.roll(x, SWEEPS, 0), y)
            stage[0, at, cs] = jnp.where(odd, top, end)
            stage[1, at, cs] = jnp.where(odd, end, top)
    near[...] = reordered(stage[0], turn)
    far[...] = reordered(stage[1], turn)


def side_by_side(parts):
    return jnp.concatenate(
        [jnp.concatenate(parts[i : i + PACK], 1) for i in range(0, len(parts), PACK)], 0
    )


def order_kernel(times, members, control, fields, pert, matrix, control_out, fields_out, pert_out):
    _, rows, width = control.shape
    turn = matrix[...]
    chunk = 2 * GROUP * PACK

    def group(step, carry):
        out = pl.ds(step * 2 * GROUP, 2 * GROUP)
        block = side_by_side([control[step * chunk + k] for k in range(chunk)])
        control_out[out] = reordered(block, turn).reshape((2 * GROUP,) + control_out.shape[1:])
        block = side_by_side(
            [pert[t, step * chunk + k] for t in range(times) for k in range(chunk)]
        )
        turned = jnp.dot(block, turn, preferred_element_type=jnp.float32)
        turned = turned.reshape((times, 2 * GROUP) + pert_out.shape[2:])
        for t in range(times):
            pert_out[t, out] = turned[t]
        return carry

    lax.fori_loop(0, members // chunk, group, 0)
    plane_kernel(fields, matrix, fields_out)


def plane_kernel(*refs):
    count = len(refs) // 2
    turn = refs[count][...]
    for ref, out in zip(refs[:count], refs[count + 1 :]):
        block = ref[...].reshape(ref.shape[0] * ref.shape[1], ref.shape[2])
        out[...] = reordered(jnp.concatenate([block] * PACK, 1), turn).reshape(out.shape)


def restore_packs(first, count, field, turn, out):
    rows, width = out.shape[1:]
    block = field[pl.ds(first, count)].reshape(count * rows, PACK * width)
    block = reordered(block, turn)
    for k in range(count):
        for b in range(PACK):
            out[(first + k) * PACK + b] = block[
                k * rows : (k + 1) * rows, b * width : (b + 1) * width
            ]


def restore_kernel(packs, field, matrix, out, token):
    turn = matrix[...]
    token[...] = jnp.zeros_like(token)
    for step in range(packs // GROUP):
        restore_packs(step * GROUP, GROUP, field, turn, out)


def coefficients_into(fields, halo_low, halo_high, base, out, ring, dims):
    cols, own = dims
    sub, n = sub_of(), own + 1
    strided = []
    for q in range(3):
        for c in range(cols):
            for i in range(own):
                ring[0, c, pl.ds(i * SUB, SUB), :] = fields[q, pl.ds(i * SUB, SUB), columns(c)]
            high, low = halo_high(base + q * SUB, c), halo_low(base + q * SUB, c)
            ring[0, c, pl.ds(own * SUB, SUB), :] = jnp.where(sub < SWEEPS, high, low)
            strided.append([ring[0, c, pl.ds(t, SUB, stride=n), :] for t in range(n)])
    for c in range(cols):
        for t in range(n):
            kappa, advect, upper = (strided[q * cols + c][t] for q in range(3))
            toward = advect * upper
            out[0, c, t] = 1.0 - 4.0 * kappa - advect
            out[1, c, t] = kappa + toward
            out[2, c, t] = kappa + (advect - toward)
            out[3, c, t] = kappa


def project_member(pert, m, rows_ref, g, total, dims):
    cols, own = dims
    out = [[list(col) for col in per_time] for per_time in total]
    for c in range(cols):
        field = [rows_ref[g, c, pl.ds(i * SUB, SUB), :] for i in range(own)]
        for t in range(len(total)):
            weight = pert[t, m, :, columns(c)]
            for i in range(own):
                out[t][c][i] = total[t][c][i] + weight[i * SUB : (i + 1) * SUB] * field[i]
    return out


def zeros(times, dims):
    cols, own = dims
    zero = jnp.zeros((SUB, LANES), jnp.float32)
    return [[[zero] * own for _ in range(cols)] for _ in range(times)]


def write_sums(ref, total, dims, lane):
    cols, own = dims
    half = LANES // PACK
    for t, per_time in enumerate(total):
        for c in range(0, cols, PACK):
            for i in range(own):
                if PACK == 1:
                    ref[pl.ds((t * own + i) * SUB, SUB), columns(c)] = per_time[c][i]
                    continue
                x, y = (per_time[c + b][i] for b in range(PACK))
                x, y = x + pltpu.roll(x, half, 1), y + pltpu.roll(y, half, 1)
                ref[pl.ds((t * own + i) * SUB, SUB), columns(c // PACK)] = jnp.where(
                    lane < half, x, y
                )


def first_kernel(dims, times, members, control, near, far, fields, pert, sums, out3,
                 halo, ring):
    cols, own = dims
    lane, sub, odd = lane_of(), sub_of(), is_odd()

    def high_of(start, c):
        rows = pl.ds(start, SUB)
        return jnp.where(odd, far[rows, columns(c)], near[rows, columns(c)])

    def low_of(start, c):
        rows = pl.ds(start, SUB)
        return jnp.where(odd, near[rows, columns(c)], far[rows, columns(c)])

    coefficients_into(
        fields, low_of, high_of, members * SWEEPS, out3, ring, dims
    )

    def group(step, total):
        for pair in range(GROUP // 2):
            first = step * GROUP + 2 * pair
            start = pl.multiple_of(first * SWEEPS, SUB)
            for c in range(cols):
                high, low = high_of(start, c), low_of(start, c)
                edges = (
                    jnp.where(sub < SWEEPS, high, pltpu.roll(low, SWEEPS, 0)),
                    jnp.where(sub < SWEEPS, pltpu.roll(high, SWEEPS, 0), low),
                )
                for k in range(2):
                    g = 2 * pair + k
                    for i in range(own):
                        rows = pl.ds(i * SUB, SUB)
                        ring[g, c, rows, :] = control[first + k, rows, columns(c)]
                    ring[g, c, pl.ds(own * SUB, SUB), :] = edges[k]
                    halo[first + k, :, columns(c)] = edges[k]
        for g in range(GROUP):
            sweeps(forward, ring, g, out3, lane, cols, own + 1)
            total = project_member(pert, step * GROUP + g, ring, g, total, dims)
        return total

    total = lax.fori_loop(0, members // GROUP, group, zeros(times, dims))
    write_sums(sums, total, dims, lane)


def pull_member(pert, m, weights, c, own):
    out = None
    for t in range(len(weights)):
        value = pert[t, m, :, columns(c)]
        terms = [value[i * SUB : (i + 1) * SUB] * weights[t][c][i] for i in range(own)]
        out = terms if out is None else [a + b for a, b in zip(out, terms)]
    return out


def gathered(parts, rows, c):
    out = parts[0][rows, columns(c)]
    for part in parts[1:]:
        out = out + part[rows, columns(c)]
    return out


def totals_of(parts, t, i, dims, lane):
    cols, own = dims
    half = LANES // PACK
    out = []
    for c in range(cols // PACK):
        x = gathered(parts, pl.ds((t * own + i) * SUB, SUB), c)
        if PACK == 1:
            out.append(x)
            continue
        y = pltpu.roll(x, half, 1)
        out += [jnp.where(lane < half, x, y), jnp.where(lane < half, y, x)]
    return out


def pulled_sweeps(step, weights, pert, ring, coef3, lane, dims):
    cols, own = dims
    for g in range(GROUP):
        for c in range(cols):
            tiles = pull_member(pert, step * GROUP + g, weights, c, own)
            for i in range(own):
                ring[g, c, pl.ds(i * SUB, SUB), :] = tiles[i]
            ring[g, c, pl.ds(own * SUB, SUB), :] = jnp.zeros((SUB, LANES), jnp.float32)
        sweeps(adjoint, ring, g, coef3, lane, cols, own + 1)


def second_kernel(dims, times, members, count, *refs):
    cols, own = dims
    parts, (innovation, weight, pert, coef3, near, far, field, spill, ring) = (
        refs[:count],
        refs[count:],
    )
    odd, lane, sub = is_odd(), lane_of(), sub_of()
    weights = []
    for t in range(times):
        weights.append([[None] * own for _ in range(cols)])
        for i in range(own):
            rows = pl.ds(i * SUB, SUB)
            total = totals_of(parts, t, i, dims, lane)
            for c in range(cols):
                weights[t][c][i] = weight[t, rows, columns(c)] * (
                    total[c] - innovation[t, rows, columns(c)]
                )

    def group(step, carry):
        pulled_sweeps(step, weights, pert, ring, coef3, lane, dims)
        for g in range(GROUP):
            m = step * GROUP + g
            for c in range(cols):
                cs = columns(c)
                tiles = [ring[g, c, pl.ds(i * SUB, SUB), :] for i in range(own + 1)]
                for i in range(own):
                    field[m, pl.ds(i * SUB, SUB), cs] = tiles[i]
                spill[m, :, cs] = tiles[own]
                low = jnp.where(sub < SWEEPS, tiles[0], tiles[own])
                high = jnp.where(sub < SWEEPS, tiles[own], tiles[own - 1])
                near[m, :, cs] = jnp.where(odd, low, high)
                far[m, :, cs] = jnp.where(odd, high, low)
        return carry

    lax.fori_loop(0, members // GROUP, group, 0)


def third_kernel(dims, times, members, control, halo, field, spill, from_near, from_far, coef3,
                 pert, gradient, sums, ring):
    cols, own = dims
    lane, sub, odd = lane_of(), sub_of(), is_odd()
    index = lax.axis_index("tile")
    inside = jnp.where(
        sub < SWEEPS,
        jnp.where(index < lax.axis_size("tile") - 1, 1.0, 0.0),
        jnp.where(index > 0, 1.0, 0.0),
    )

    def group(step, carry):
        total, square = carry
        for g in range(GROUP):
            m = step * GROUP + g
            for c in range(cols):
                cs = columns(c)
                a, b = from_near[m, :, cs], from_far[m, :, cs]
                high, low = jnp.where(odd, b, a), jnp.where(odd, a, b)
                for i in range(own):
                    rows = pl.ds(i * SUB, SUB)
                    value = control[m, rows, cs] + field[m, rows, cs]
                    if i == 0:
                        value = value + jnp.where(sub < SWEEPS, low, 0.0)
                    if i == own - 1:
                        value = value + jnp.where(sub < SWEEPS, 0.0, high)
                    gradient[m, rows, cs] = value
                    ring[g, c, rows, :] = value
                    square = square + value * value
                edge = jnp.where(sub < SWEEPS, high, low) + spill[m, :, cs]
                ring[g, c, pl.ds(own * SUB, SUB), :] = inside * (halo[m, :, cs] + edge)
        for g in range(GROUP):
            sweeps(forward, ring, g, coef3, lane, cols, own + 1)
            total = project_member(pert, step * GROUP + g, ring, g, total, dims)
        return total, square

    total, square = lax.fori_loop(
        0,
        members // GROUP,
        group,
        (zeros(times, dims), jnp.zeros((SUB, LANES), jnp.float32)),
    )
    write_sums(sums, total, dims, lane)
    sums[pl.ds(times * own * SUB, SUB), :] = jnp.zeros((SUB, sums.shape[1]), jnp.float32)
    sums[pl.ds(times * own * SUB, SUB), columns(0)] = square


def fourth_kernel(dims, times, members, count, *refs):
    cols, own = dims
    parts, (weight, pert, _, coef3, gradient, field, near, far, ring) = refs[:count], refs[count:]
    odd, sub, lane = is_odd(), sub_of(), lane_of()
    weights = []
    curve = jnp.zeros((SUB, LANES), jnp.float32)
    for t in range(times):
        weights.append([[None] * own for _ in range(cols)])
        for i in range(own):
            total = totals_of(parts, t, i, dims, lane)
            for c in range(cols):
                weights[t][c][i] = weight[t, pl.ds(i * SUB, SUB), columns(c)] * total[c]
                curve = curve + total[c] * weights[t][c][i]
    square = gathered(parts, pl.ds(times * own * SUB, SUB), 0)
    base = members * SWEEPS
    near[pl.ds(base, 2 * SUB), :] = jnp.zeros((2 * SUB, near.shape[1]), jnp.float32)
    near[pl.ds(base, SUB), columns(0)] = square
    near[pl.ds(base + SUB, SUB), columns(0)] = curve * (1.0 / PACK)

    def group(step, carry):
        pulled_sweeps(step, weights, pert, ring, coef3, lane, dims)
        for pair in range(GROUP // 2):
            first = step * GROUP + 2 * pair
            start = pl.multiple_of(first * SWEEPS, SUB)
            for c in range(cols):
                cs = columns(c)
                for k in range(2):
                    for i in range(own):
                        rows = pl.ds(i * SUB, SUB)
                        field[first + k, rows, cs] = (
                            gradient[first + k, rows, cs] + ring[2 * pair + k, c, rows, :]
                        )
                x, y = (ring[2 * pair + k, c, pl.ds(own * SUB, SUB), :] for k in range(2))
                high = jnp.where(sub < SWEEPS, x, pltpu.roll(y, SWEEPS, 0))
                low = jnp.where(sub < SWEEPS, pltpu.roll(x, SWEEPS, 0), y)
                near[pl.ds(start, SUB), cs] = jnp.where(odd, low, high)
                far[pl.ds(start, SUB), cs] = jnp.where(odd, high, low)
        return carry

    lax.fori_loop(0, members // GROUP, group, 0)


def fifth_kernel(dims, members, field, near, far, matrix, product, token, whole):
    token[...] = jnp.zeros_like(token)
    cols, own = dims
    sub, odd = sub_of(), is_odd()
    turn = matrix[...]

    def group(step):
        for pair in range(GROUP // 2):
            first = step * GROUP + 2 * pair
            start = first * SWEEPS
            rows8 = pl.ds(start if isinstance(step, int) else pl.multiple_of(start, SUB), SUB)
            for c in range(cols):
                cs = columns(c)
                a, b = near[rows8, cs], far[rows8, cs]
                high, low = jnp.where(odd, b, a), jnp.where(odd, a, b)
                lows = (low, pltpu.roll(low, SWEEPS, 0))
                highs = (pltpu.roll(high, SWEEPS, 0), high)
                for k in range(2):
                    for i in range(own):
                        rows = pl.ds(i * SUB, SUB)
                        value = field[first + k, rows, cs]
                        if i == 0:
                            value = value + jnp.where(sub < SWEEPS, lows[k], 0.0)
                        if i == own - 1:
                            value = value + jnp.where(sub < SWEEPS, 0.0, highs[k])
                        whole[first + k, rows, cs] = value

    def both(step, carry):
        restore_packs((step - 1) * GROUP, GROUP, whole, turn, product)
        group(step)
        return carry

    group(0)
    lax.fori_loop(1, members // GROUP, both, 0, unroll=UNROLL)
    restore_packs(members - GROUP, GROUP, whole, turn, product)


def length_kernel(*refs):
    scalars, length = refs[:-2], refs[-1]
    total = sum((ref[...] for ref in scalars[1:]), scalars[0][...])
    square, curve = (
        jnp.sum(jnp.sum(x, axis=0, keepdims=True), axis=1, keepdims=True)
        for x in (total[:SUB], total[SUB:])
    )
    length[...] = square / (square + curve)


def bind(kernel, *static):
    def bound(*refs):
        kernel(*static, *refs)

    return bound


def shards(perturbations, control, innovation, obs_weight, diffusion, advection, upwind):
    times, members, rows, width = perturbations.shape
    packs, wide = members // PACK, PACK * width
    cols, own = wide // LANES, rows // SUB
    dims = (cols, own)

    turn, back = order(width, False), order(width, True)
    edge = f32(packs * SWEEPS + 3 * SUB, wide)
    planes = f32(3, rows, width)
    near, far, fields = call(
        bind(edge_kernel, members),
        [edge, edge, planes],
        [
            pltpu.VMEM(control.shape, jnp.float32),
            pltpu.VMEM((rows, width), jnp.int32),
            pltpu.VMEM((2,) + edge.shape, jnp.float32),
            pltpu.SemaphoreType.DMA((CHUNKS + 3,)),
        ],
        [control, diffusion, advection, upwind],
        near=-4,
        limit=VMEM_BYTES - 4 * (2 * edge.size + planes.size + SPARE),
    )
    near, far = swap(near, far)
    packed = f32(packs, rows, wide)
    per_time = f32(times, rows, wide)
    gradient_shape = f32(*control.shape)
    control, fields, perturbations = call(
        bind(order_kernel, times, members),
        [packed, f32(3, rows, wide), f32(times, *packed.shape)],
        [],
        [control, fields, perturbations, turn],
        flops=2_000_000_000,
    )
    innovation, obs_weight = call(
        plane_kernel, [per_time, per_time], [], [innovation, obs_weight, turn], flops=200_000_000
    )

    def ring_of(n):
        return pltpu.VMEM((GROUP, cols, n * SUB, LANES), jnp.float32)

    sums, coef3, halo = call(
        bind(first_kernel, dims, times, packs),
        [
            f32(times * rows, width),
            f32(4, cols, own + 1, SUB, LANES),
            f32(packs, SUB, wide),
        ],
        [ring_of(own + 1)],
        [control, near, far, fields, perturbations],
        flops=4_000_000_000,
    )
    parts = [sums] + others(sums, "mem")
    edges = f32(packs, SUB, wide)
    near, far, field, spill = call(
        bind(second_kernel, dims, times, packs, len(parts)),
        [edges, edges, packed, edges],
        [ring_of(own + 1)],
        parts + [innovation, obs_weight, perturbations, coef3],
    )
    from_near, from_far = swap(near, far)
    gradient, sums = call(
        bind(third_kernel, dims, times, packs),
        [packed, f32(times * rows + SUB, width)],
        [ring_of(own + 1)],
        [control, halo, field, spill, from_near, from_far, coef3, perturbations],
        flops=4_000_000_000,
    )
    parts = [sums] + others(sums, "mem")
    restored, token = call(
        bind(restore_kernel, packs),
        [gradient_shape, f32(SUB, LANES)],
        [],
        [gradient, back],
        flops=1_000_000_000,
    )
    field, near, far = call(
        bind(fourth_kernel, dims, times, packs, len(parts)),
        [packed, f32(packs * SWEEPS + 2 * SUB, wide), f32(packs * SWEEPS, wide)],
        [ring_of(own + 1)],
        parts + [obs_weight, perturbations, token, coef3, gradient],
    )
    from_near, from_far = swap(near, far)
    one = near[packs * SWEEPS :, :LANES] + from_near[packs * SWEEPS :, :LANES]
    scalars = [one] + others(one, "tile", 2)
    product, token = call(
        bind(fifth_kernel, dims, packs),
        [gradient_shape, f32(SUB, LANES)],
        [pltpu.VMEM(gradient.shape, jnp.float32)],
        [field, from_near, from_far, back],
        flops=1_000_000_000,
    )
    (length,) = call(length_kernel, [f32(1, 1)], [], scalars + [token])
    return restored, product, length[0, 0]


def solution(mesh):
    return jax.shard_map(
        shards,
        mesh=mesh,
        in_specs=(
            P(None, "mem", "tile", None),
            P("mem", "tile", None),
            P(None, "tile", None),
            P(None, "tile", None),
            P("tile", None),
            P("tile", None),
            P("tile", None),
        ),
        out_specs=(P("mem", "tile", None), P("mem", "tile", None), P()),
        check_vma=False,
    )
```

```python
import functools
import jax
import jax.numpy as jnp
from jax import lax
from jax.experimental import pallas as pl
from jax.experimental.pallas import tpu as pltpu
from jax.sharding import PartitionSpec as P

SWEEPS = 4
SUB = 8
CHUNKS = 4
UNROLL = 7
PIECES = 2
VMEM_BYTES = 67043328
SPARE = 3072
LANES = 128
PACK = 1
GROUP = 8


def pairs_inner(count):
    return [(i, i ^ 1) for i in range(count) if (i ^ 1) < count]


def pairs_outer(count):
    partner = [(i, i + 1 if i % 2 else i - 1) for i in range(count)]
    return [(i, j) for i, j in partner if 0 <= j < count]


def swap(inner, outer):
    count = lax.axis_size("tile")
    far = lax.ppermute(outer, "tile", pairs_outer(count))
    near = lax.ppermute(inner, "tile", pairs_inner(count))
    return near, far


def others(value, axis, stride=1):
    count = lax.axis_size(axis)
    power = count & (count - 1) == 0
    return [
        lax.ppermute(
            value, axis, [(i, i ^ step if power else (i + step) % count) for i in range(count)]
        )
        for step in reversed(range(stride, count, stride))
    ]


def order(width, back):
    wide = PACK * width
    cols, each = wide // LANES, LANES // PACK
    a = jnp.arange(wide, dtype=jnp.int32)
    lane, vector = a % LANES, a // LANES
    source = (lane // each) * width + cols * (lane % each) + vector
    if back:
        return (source[:, None] == a[None, :]).astype(jnp.bfloat16)
    return (a[:, None] == source[None, :]).astype(jnp.bfloat16)


def order_matrix(width):
    wide = PACK * width
    cols, each = wide // LANES, LANES // PACK
    a = lax.broadcasted_iota(jnp.int32, (wide, wide), 1)
    lane, vector = a % LANES, a // LANES
    source = (lane // each) * width + cols * (lane % each) + vector
    return jnp.where(lax.broadcasted_iota(jnp.int32, (wide, wide), 0) == source, 1.0, 0.0).astype(
        jnp.bfloat16
    )


def reordered(x, matrix):
    high = x.astype(jnp.bfloat16)
    low = (x - high.astype(jnp.float32)).astype(jnp.bfloat16)
    return jnp.dot(high, matrix, preferred_element_type=jnp.float32) + jnp.dot(
        low, matrix, preferred_element_type=jnp.float32
    )


def columns(c):
    return pl.ds(c * LANES, LANES)


def sides(values, lane):
    last, each = len(values) - 1, LANES // PACK
    right = jnp.where(lane % each == each - 1, 0.0, pltpu.roll(values[0], LANES - 1, 1))
    left = jnp.where(lane % each == 0, 0.0, pltpu.roll(values[last], 1, 1))
    around = [left] + list(values) + [right]
    return [around[c] + around[c + 2] for c in range(last + 1)]


def below_of(x):
    return x[1:] + [pltpu.roll(x[0], SUB - 1, 0)]


def above_of(x):
    return [pltpu.roll(x[-1], 1, 0)] + x[:-1]


def forward(x, coef, lane):
    cols, tiles = len(x), len(x[0])
    lateral = [sides([x[c][t] for c in range(cols)], lane) for t in range(tiles)]
    out = []
    for c in range(cols):
        below, above = below_of(x[c]), above_of(x[c])
        out.append(
            [
                coef[0, c, t] * x[c][t]
                + coef[1, c, t] * below[t]
                + coef[2, c, t] * above[t]
                + coef[3, c, t] * lateral[t][c]
                for t in range(tiles)
            ]
        )
    return out


def adjoint(x, coef, lane):
    cols, tiles = len(x), len(x[0])
    lateral = [
        sides([coef[3, c, t] * x[c][t] for c in range(cols)], lane) for t in range(tiles)
    ]
    out = []
    for c in range(cols):
        below = below_of([coef[2, c, t] * x[c][t] for t in range(tiles)])
        above = above_of([coef[1, c, t] * x[c][t] for t in range(tiles)])
        out.append(
            [
                coef[0, c, t] * x[c][t] + below[t] + above[t] + lateral[t][c]
                for t in range(tiles)
            ]
        )
    return out


def sweeps(step, rows_ref, g, coef, lane, cols, tiles):
    x = [
        [rows_ref[g, c, pl.ds(t, SUB, stride=tiles), :] for t in range(tiles)]
        for c in range(cols)
    ]
    for _ in range(SWEEPS):
        x = step(x, coef, lane)
    for c in range(cols):
        for t in range(tiles):
            rows_ref[g, c, pl.ds(t, SUB, stride=tiles), :] = x[c][t]


def lane_of():
    return lax.broadcasted_iota(jnp.int32, (SUB, LANES), 1)


def sub_of():
    return lax.broadcasted_iota(jnp.int32, (SUB, LANES), 0)


def is_odd():
    return lax.axis_index("tile") % 2 == 1


def call(kernel, outs, scratch, operands, near=None, flops=1, limit=24 * 2**20):
    near = len(operands) if near is None else len(operands) + near
    nbytes = sum(x.size * x.dtype.itemsize for x in operands)
    return pl.pallas_call(
        kernel,
        out_shape=outs,
        in_specs=[
            pl.BlockSpec(memory_space=pltpu.VMEM if k < near else pl.ANY)
            for k in range(len(operands))
        ],
        out_specs=[pl.BlockSpec(memory_space=pltpu.VMEM)] * len(outs),
        scratch_shapes=scratch,
        compiler_params=pltpu.CompilerParams(vmem_limit_bytes=limit),
        cost_estimate=pl.CostEstimate(flops=flops, bytes_accessed=nbytes, transcendentals=0),
    )(*operands)


def f32(*shape):
    return jax.ShapeDtypeStruct(shape, jnp.float32)


def edge_kernel(members, control, diffusion, advection, upwind, near, far, fields, buf, number,
                stage, sems):
    _, rows, width = control.shape
    chunk = members // CHUNKS
    copies = [
        pltpu.make_async_copy(
            control.at[pl.ds(i * chunk, chunk)], buf.at[pl.ds(i * chunk, chunk)], sems.at[i]
        )
        for i in range(CHUNKS)
    ] + [
        pltpu.make_async_copy(diffusion, fields.at[0], sems.at[CHUNKS]),
        pltpu.make_async_copy(advection, fields.at[1], sems.at[CHUNKS + 1]),
        pltpu.make_async_copy(upwind, number, sems.at[CHUNKS + 2]),
    ]
    for copy in copies[CHUNKS:] + copies[:CHUNKS]:
        copy.start()
    odd, turn = is_odd(), order_matrix(width)
    sub = lax.broadcasted_iota(jnp.int32, (SUB, width), 0)
    last = pl.ds(rows - SUB, SUB)
    for copy in copies[CHUNKS:]:
        copy.wait()
    fields[2] = number[...].astype(jnp.float32)
    for q in range(3):
        top, end = fields[q, pl.ds(0, SUB), :], fields[q, last, :]
        at = pl.ds(members // PACK * SWEEPS + q * SUB, SUB)
        for b in range(PACK):
            cs = pl.ds(b * width, width)
            stage[0, at, cs] = jnp.where(odd, top, end)
            stage[1, at, cs] = jnp.where(odd, end, top)
    pairs = chunk // (2 * PACK)
    for k in range(members // (2 * PACK)):
        if k % pairs == 0:
            copies[k // pairs].wait()
        at = pl.ds(k * SUB, SUB)
        for b in range(PACK):
            first, second = 2 * PACK * k + b, 2 * PACK * k + PACK + b
            cs = pl.ds(b * width, width)
            x, y = buf[first, pl.ds(0, SUB), :], buf[second, pl.ds(0, SUB), :]
            top = jnp.where(sub < SWEEPS, x, pltpu.roll(y, SWEEPS, 0))
            x, y = buf[first, last, :], buf[second, last, :]
            end = jnp.where(sub < SWEEPS, pltpu.roll(x, SWEEPS, 0), y)
            stage[0, at, cs] = jnp.where(odd, top, end)
            stage[1, at, cs] = jnp.where(odd, end, top)
    near[...] = reordered(stage[0], turn)
    far[...] = reordered(stage[1], turn)


def side_by_side(parts):
    return jnp.concatenate(
        [jnp.concatenate(parts[i : i + PACK], 1) for i in range(0, len(parts), PACK)], 0
    )


def order_kernel(times, members, control, fields, pert, matrix, control_out, fields_out, pert_out):
    _, rows, width = control.shape
    turn = matrix[...]
    chunk = 2 * GROUP * PACK

    def group(step, carry):
        out = pl.ds(step * 2 * GROUP, 2 * GROUP)
        block = side_by_side([control[step * chunk + k] for k in range(chunk)])
        control_out[out] = reordered(block, turn).reshape((2 * GROUP,) + control_out.shape[1:])
        block = side_by_side(
            [pert[t, step * chunk + k] for t in range(times) for k in range(chunk)]
        )
        turned = jnp.dot(block, turn, preferred_element_type=jnp.float32)
        turned = turned.reshape((times, 2 * GROUP) + pert_out.shape[2:])
        for t in range(times):
            pert_out[t, out] = turned[t]
        return carry

    lax.fori_loop(0, members // chunk, group, 0)
    plane_kernel(fields, matrix, fields_out)


def plane_kernel(*refs):
    count = len(refs) // 2
    turn = refs[count][...]
    for ref, out in zip(refs[:count], refs[count + 1 :]):
        block = ref[...].reshape(ref.shape[0] * ref.shape[1], ref.shape[2])
        out[...] = reordered(jnp.concatenate([block] * PACK, 1), turn).reshape(out.shape)


def restore_packs(first, count, field, turn, out, offset=0):
    rows, width = out.shape[1:]
    block = field[pl.ds(first, count)].reshape(count * rows, PACK * width)
    block = reordered(block, turn)
    for k in range(count):
        for b in range(PACK):
            out[(offset + first + k) * PACK + b] = block[
                k * rows : (k + 1) * rows, b * width : (b + 1) * width
            ]


def restore_kernel(packs, matrix, *refs):
    fields, (out, token) = refs[:-2], refs[-2:]
    turn = matrix[...]
    token[...] = jnp.zeros_like(token)
    part = packs // len(fields)
    for k, field in enumerate(fields):
        for step in range(part // GROUP):
            restore_packs(step * GROUP, GROUP, field, turn, out, k * part)


def coefficients_into(fields, halo_low, halo_high, base, out, ring, dims):
    cols, own = dims
    sub, n = sub_of(), own + 1
    strided = []
    for q in range(3):
        for c in range(cols):
            for i in range(own):
                ring[0, c, pl.ds(i * SUB, SUB), :] = fields[q, pl.ds(i * SUB, SUB), columns(c)]
            high, low = halo_high(base + q * SUB, c), halo_low(base + q * SUB, c)
            ring[0, c, pl.ds(own * SUB, SUB), :] = jnp.where(sub < SWEEPS, high, low)
            strided.append([ring[0, c, pl.ds(t, SUB, stride=n), :] for t in range(n)])
    for c in range(cols):
        for t in range(n):
            kappa, advect, upper = (strided[q * cols + c][t] for q in range(3))
            toward = advect * upper
            out[0, c, t] = 1.0 - 4.0 * kappa - advect
            out[1, c, t] = kappa + toward
            out[2, c, t] = kappa + (advect - toward)
            out[3, c, t] = kappa


def project_member(pert, m, rows_ref, g, total, dims):
    cols, own = dims
    out = [[list(col) for col in per_time] for per_time in total]
    for c in range(cols):
        field = [rows_ref[g, c, pl.ds(i * SUB, SUB), :] for i in range(own)]
        for t in range(len(total)):
            weight = pert[t, m, :, columns(c)]
            for i in range(own):
                out[t][c][i] = total[t][c][i] + weight[i * SUB : (i + 1) * SUB] * field[i]
    return out


def zeros(times, dims):
    cols, own = dims
    zero = jnp.zeros((SUB, LANES), jnp.float32)
    return [[[zero] * own for _ in range(cols)] for _ in range(times)]


def write_sums(ref, total, dims, lane):
    cols, own = dims
    half = LANES // PACK
    for t, per_time in enumerate(total):
        for c in range(0, cols, PACK):
            for i in range(own):
                if PACK == 1:
                    ref[pl.ds((t * own + i) * SUB, SUB), columns(c)] = per_time[c][i]
                    continue
                x, y = (per_time[c + b][i] for b in range(PACK))
                x, y = x + pltpu.roll(x, half, 1), y + pltpu.roll(y, half, 1)
                ref[pl.ds((t * own + i) * SUB, SUB), columns(c // PACK)] = jnp.where(
                    lane < half, x, y
                )


def first_kernel(dims, times, members, control, near, far, fields, pert, sums, out3,
                 halo, ring):
    cols, own = dims
    lane, sub, odd = lane_of(), sub_of(), is_odd()

    def high_of(start, c):
        rows = pl.ds(start, SUB)
        return jnp.where(odd, far[rows, columns(c)], near[rows, columns(c)])

    def low_of(start, c):
        rows = pl.ds(start, SUB)
        return jnp.where(odd, near[rows, columns(c)], far[rows, columns(c)])

    coefficients_into(
        fields, low_of, high_of, members * SWEEPS, out3, ring, dims
    )

    def group(step, total):
        for pair in range(GROUP // 2):
            first = step * GROUP + 2 * pair
            start = pl.multiple_of(first * SWEEPS, SUB)
            for c in range(cols):
                high, low = high_of(start, c), low_of(start, c)
                edges = (
                    jnp.where(sub < SWEEPS, high, pltpu.roll(low, SWEEPS, 0)),
                    jnp.where(sub < SWEEPS, pltpu.roll(high, SWEEPS, 0), low),
                )
                for k in range(2):
                    g = 2 * pair + k
                    for i in range(own):
                        rows = pl.ds(i * SUB, SUB)
                        ring[g, c, rows, :] = control[first + k, rows, columns(c)]
                    ring[g, c, pl.ds(own * SUB, SUB), :] = edges[k]
                    halo[first + k, :, columns(c)] = edges[k]
        for g in range(GROUP):
            sweeps(forward, ring, g, out3, lane, cols, own + 1)
            total = project_member(pert, step * GROUP + g, ring, g, total, dims)
        return total

    total = lax.fori_loop(0, members // GROUP, group, zeros(times, dims))
    write_sums(sums, total, dims, lane)


def pull_member(pert, m, weights, c, own):
    out = None
    for t in range(len(weights)):
        value = pert[t, m, :, columns(c)]
        terms = [value[i * SUB : (i + 1) * SUB] * weights[t][c][i] for i in range(own)]
        out = terms if out is None else [a + b for a, b in zip(out, terms)]
    return out


def gathered(parts, rows, c):
    out = parts[0][rows, columns(c)]
    for part in parts[1:]:
        out = out + part[rows, columns(c)]
    return out


def totals_of(parts, t, i, dims, lane):
    cols, own = dims
    half = LANES // PACK
    out = []
    for c in range(cols // PACK):
        x = gathered(parts, pl.ds((t * own + i) * SUB, SUB), c)
        if PACK == 1:
            out.append(x)
            continue
        y = pltpu.roll(x, half, 1)
        out += [jnp.where(lane < half, x, y), jnp.where(lane < half, y, x)]
    return out


def pulled_sweeps(start, weights, pert, ring, coef3, lane, dims):
    cols, own = dims
    for g in range(GROUP):
        for c in range(cols):
            tiles = pull_member(pert, start + g, weights, c, own)
            for i in range(own):
                ring[g, c, pl.ds(i * SUB, SUB), :] = tiles[i]
            ring[g, c, pl.ds(own * SUB, SUB), :] = jnp.zeros((SUB, LANES), jnp.float32)
        sweeps(adjoint, ring, g, coef3, lane, cols, own + 1)


def second_kernel(dims, times, members, offset, count, *refs):
    cols, own = dims
    parts, (innovation, weight, pert, coef3, near, far, field, spill, ring) = (
        refs[:count],
        refs[count:],
    )
    odd, lane, sub = is_odd(), lane_of(), sub_of()
    weights = []
    for t in range(times):
        weights.append([[None] * own for _ in range(cols)])
        for i in range(own):
            rows = pl.ds(i * SUB, SUB)
            total = totals_of(parts, t, i, dims, lane)
            for c in range(cols):
                weights[t][c][i] = weight[t, rows, columns(c)] * (
                    total[c] - innovation[t, rows, columns(c)]
                )

    def group(step, carry):
        pulled_sweeps(offset + step * GROUP, weights, pert, ring, coef3, lane, dims)
        for g in range(GROUP):
            m = step * GROUP + g
            for c in range(cols):
                cs = columns(c)
                tiles = [ring[g, c, pl.ds(i * SUB, SUB), :] for i in range(own + 1)]
                for i in range(own):
                    field[m, pl.ds(i * SUB, SUB), cs] = tiles[i]
                spill[m, :, cs] = tiles[own]
                low = jnp.where(sub < SWEEPS, tiles[0], tiles[own])
                high = jnp.where(sub < SWEEPS, tiles[own], tiles[own - 1])
                near[m, :, cs] = jnp.where(odd, low, high)
                far[m, :, cs] = jnp.where(odd, high, low)
        return carry

    lax.fori_loop(0, members // GROUP, group, 0)


def third_kernel(dims, times, members, offset, control, halo, field, spill, from_near, from_far,
                 coef3, pert, *refs):
    gradient, sums, ring = refs[-3:]
    cols, own = dims
    lane, sub, odd = lane_of(), sub_of(), is_odd()
    index = lax.axis_index("tile")
    inside = jnp.where(
        sub < SWEEPS,
        jnp.where(index < lax.axis_size("tile") - 1, 1.0, 0.0),
        jnp.where(index > 0, 1.0, 0.0),
    )

    def group(step, carry):
        total, square = carry
        for g in range(GROUP):
            m = step * GROUP + g
            for c in range(cols):
                cs = columns(c)
                a, b = from_near[m, :, cs], from_far[m, :, cs]
                high, low = jnp.where(odd, b, a), jnp.where(odd, a, b)
                for i in range(own):
                    rows = pl.ds(i * SUB, SUB)
                    value = control[offset + m, rows, cs] + field[m, rows, cs]
                    if i == 0:
                        value = value + jnp.where(sub < SWEEPS, low, 0.0)
                    if i == own - 1:
                        value = value + jnp.where(sub < SWEEPS, 0.0, high)
                    gradient[m, rows, cs] = value
                    ring[g, c, rows, :] = value
                    square = square + value * value
                edge = jnp.where(sub < SWEEPS, high, low) + spill[m, :, cs]
                ring[g, c, pl.ds(own * SUB, SUB), :] = inside * (halo[offset + m, :, cs] + edge)
        for g in range(GROUP):
            sweeps(forward, ring, g, coef3, lane, cols, own + 1)
            total = project_member(pert, offset + step * GROUP + g, ring, g, total, dims)
        return total, square

    total, square = lax.fori_loop(
        0,
        members // GROUP,
        group,
        (zeros(times, dims), jnp.zeros((SUB, LANES), jnp.float32)),
    )
    write_sums(sums, total, dims, lane)
    sums[pl.ds(times * own * SUB, SUB), :] = jnp.zeros((SUB, sums.shape[1]), jnp.float32)
    sums[pl.ds(times * own * SUB, SUB), columns(0)] = square
    for before in refs[:-3]:
        sums[...] = sums[...] + before[...]


def tie_kernel(value, _, out):
    out[...] = value[...]


def fourth_kernel(dims, times, members, count, *refs):
    cols, own = dims
    parts, (weight, pert, _, coef3, *refs) = refs[:count], refs[count:]
    gradients, (field, near, far, ring) = refs[:-4], refs[-4:]
    odd, sub, lane = is_odd(), sub_of(), lane_of()
    weights = []
    curve = jnp.zeros((SUB, LANES), jnp.float32)
    for t in range(times):
        weights.append([[None] * own for _ in range(cols)])
        for i in range(own):
            total = totals_of(parts, t, i, dims, lane)
            for c in range(cols):
                weights[t][c][i] = weight[t, pl.ds(i * SUB, SUB), columns(c)] * total[c]
                curve = curve + total[c] * weights[t][c][i]
    square = gathered(parts, pl.ds(times * own * SUB, SUB), 0)
    base = members * SWEEPS
    near[pl.ds(base, 2 * SUB), :] = jnp.zeros((2 * SUB, near.shape[1]), jnp.float32)
    near[pl.ds(base, SUB), columns(0)] = square
    near[pl.ds(base + SUB, SUB), columns(0)] = curve * (1.0 / PACK)

    def group(offset, gradient, step, carry):
        pulled_sweeps(offset + step * GROUP, weights, pert, ring, coef3, lane, dims)
        for pair in range(GROUP // 2):
            here = step * GROUP + 2 * pair
            first = offset + here
            start = pl.multiple_of(first * SWEEPS, SUB)
            for c in range(cols):
                cs = columns(c)
                for k in range(2):
                    for i in range(own):
                        rows = pl.ds(i * SUB, SUB)
                        field[first + k, rows, cs] = (
                            gradient[here + k, rows, cs] + ring[2 * pair + k, c, rows, :]
                        )
                x, y = (ring[2 * pair + k, c, pl.ds(own * SUB, SUB), :] for k in range(2))
                high = jnp.where(sub < SWEEPS, x, pltpu.roll(y, SWEEPS, 0))
                low = jnp.where(sub < SWEEPS, pltpu.roll(x, SWEEPS, 0), y)
                near[pl.ds(start, SUB), cs] = jnp.where(odd, low, high)
                far[pl.ds(start, SUB), cs] = jnp.where(odd, high, low)
        return carry

    part = members // len(gradients)
    for k, gradient in enumerate(gradients):
        lax.fori_loop(0, part // GROUP, functools.partial(group, k * part, gradient), 0)


def fifth_kernel(dims, members, field, near, far, matrix, product, token, whole):
    token[...] = jnp.zeros_like(token)
    cols, own = dims
    sub, odd = sub_of(), is_odd()
    turn = matrix[...]

    def group(step):
        for pair in range(GROUP // 2):
            first = step * GROUP + 2 * pair
            start = first * SWEEPS
            rows8 = pl.ds(start if isinstance(step, int) else pl.multiple_of(start, SUB), SUB)
            for c in range(cols):
                cs = columns(c)
                a, b = near[rows8, cs], far[rows8, cs]
                high, low = jnp.where(odd, b, a), jnp.where(odd, a, b)
                lows = (low, pltpu.roll(low, SWEEPS, 0))
                highs = (pltpu.roll(high, SWEEPS, 0), high)
                for k in range(2):
                    for i in range(own):
                        rows = pl.ds(i * SUB, SUB)
                        value = field[first + k, rows, cs]
                        if i == 0:
                            value = value + jnp.where(sub < SWEEPS, lows[k], 0.0)
                        if i == own - 1:
                            value = value + jnp.where(sub < SWEEPS, 0.0, highs[k])
                        whole[first + k, rows, cs] = value

    def both(step, carry):
        restore_packs((step - 1) * GROUP, GROUP, whole, turn, product)
        group(step)
        return carry

    group(0)
    lax.fori_loop(1, members // GROUP, both, 0, unroll=UNROLL)
    restore_packs(members - GROUP, GROUP, whole, turn, product)


def length_kernel(*refs):
    scalars, length = refs[:-2], refs[-1]
    total = sum((ref[...] for ref in scalars[1:]), scalars[0][...])
    square, curve = (
        jnp.sum(jnp.sum(x, axis=0, keepdims=True), axis=1, keepdims=True)
        for x in (total[:SUB], total[SUB:])
    )
    length[...] = square / (square + curve)


def bind(kernel, *static):
    def bound(*refs):
        kernel(*static, *refs)

    return bound


def shards(perturbations, control, innovation, obs_weight, diffusion, advection, upwind):
    times, members, rows, width = perturbations.shape
    packs, wide = members // PACK, PACK * width
    cols, own = wide // LANES, rows // SUB
    dims = (cols, own)

    turn, back = order(width, False), order(width, True)
    edge = f32(packs * SWEEPS + 3 * SUB, wide)
    planes = f32(3, rows, width)
    near, far, fields = call(
        bind(edge_kernel, members),
        [edge, edge, planes],
        [
            pltpu.VMEM(control.shape, jnp.float32),
            pltpu.VMEM((rows, width), jnp.int32),
            pltpu.VMEM((2,) + edge.shape, jnp.float32),
            pltpu.SemaphoreType.DMA((CHUNKS + 3,)),
        ],
        [control, diffusion, advection, upwind],
        near=-4,
        limit=VMEM_BYTES - 4 * (2 * edge.size + planes.size + SPARE),
    )
    near, far = swap(near, far)
    packed = f32(packs, rows, wide)
    per_time = f32(times, rows, wide)
    gradient_shape = f32(*control.shape)
    control, fields, perturbations = call(
        bind(order_kernel, times, members),
        [packed, f32(3, rows, wide), f32(times, *packed.shape)],
        [],
        [control, fields, perturbations, turn],
        flops=2_000_000_000,
    )
    innovation, obs_weight = call(
        plane_kernel, [per_time, per_time], [], [innovation, obs_weight, turn], flops=200_000_000
    )

    def ring_of(n):
        return pltpu.VMEM((GROUP, cols, n * SUB, LANES), jnp.float32)

    sums, coef3, halo = call(
        bind(first_kernel, dims, times, packs),
        [
            f32(times * rows, width),
            f32(4, cols, own + 1, SUB, LANES),
            f32(packs, SUB, wide),
        ],
        [ring_of(own + 1)],
        [control, near, far, fields, perturbations],
        flops=4_000_000_000,
    )
    parts = [sums] + others(sums, "mem")
    half = packs // PIECES
    pieces = []
    for k in range(PIECES):
        edges, some = f32(half, SUB, wide), f32(half, rows, wide)
        near, far, field, spill = call(
            bind(second_kernel, dims, times, half, k * half, len(parts)),
            [edges, edges, some, edges],
            [ring_of(own + 1)],
            parts + [innovation, obs_weight, perturbations, coef3],
            flops=2_000_000_000,
        )
        if k:
            (near,) = call(tie_kernel, [edges], [], [near, pieces[-1][3]])
        pieces.append([field, spill] + list(swap(near, far)))
    gradients, before = [], []
    for k in range(PIECES):
        gradient, sums = call(
            bind(third_kernel, dims, times, half, k * half),
            [some, f32(times * rows + SUB, width)],
            [ring_of(own + 1)],
            [control, halo] + pieces[k] + [coef3, perturbations] + before,
            flops=2_000_000_000,
        )
        gradients.append(gradient)
        before = [sums]
    parts = [sums] + others(sums, "mem")
    restored, token = call(
        bind(restore_kernel, packs),
        [gradient_shape, f32(SUB, LANES)],
        [],
        [back] + gradients,
        flops=1_000_000_000,
    )
    field, near, far = call(
        bind(fourth_kernel, dims, times, packs, len(parts)),
        [packed, f32(packs * SWEEPS + 2 * SUB, wide), f32(packs * SWEEPS, wide)],
        [ring_of(own + 1)],
        parts + [obs_weight, perturbations, token, coef3] + gradients,
    )
    from_near, from_far = swap(near, far)
    one = near[packs * SWEEPS :, :LANES] + from_near[packs * SWEEPS :, :LANES]
    scalars = [one] + others(one, "tile", 2)
    product, token = call(
        bind(fifth_kernel, dims, packs),
        [gradient_shape, f32(SUB, LANES)],
        [pltpu.VMEM(packed.shape, jnp.float32)],
        [field, from_near, from_far, back],
        flops=1_000_000_000,
    )
    (length,) = call(length_kernel, [f32(1, 1)], [], scalars + [token])
    return restored, product, length[0, 0]


def solution(mesh):
    return jax.shard_map(
        shards,
        mesh=mesh,
        in_specs=(
            P(None, "mem", "tile", None),
            P("mem", "tile", None),
            P(None, "tile", None),
            P(None, "tile", None),
            P("tile", None),
            P("tile", None),
            P("tile", None),
        ),
        out_specs=(P("mem", "tile", None), P("mem", "tile", None), P()),
        check_vma=False,
    )
```
